256 devices in a mesh: gx: 8 (over z_hi, core), gy: 4 (over y), gz: 8 (over z_lo, x).
Axes of the slice: x: 4, y: 4, z: 8 (z_hi: 4, z_lo: 2; z = z_hi * 2 + z_lo), core: 2. Of those that a mesh axis runs over, the one named last changes fastest.
Arguments:
- field: float32 [256, 1024, 512], P('gz', 'gx', 'gy'), may hold values from -48 to 48
- factor_a: float32 [1024, 1024], replicated, may hold values from -0.5 to 3.5
- factor_b: float32 [512, 512], replicated, may hold values from -0.5 to 3.5
- factor_c: float32 [256, 256], replicated, may hold values from -0.5 to 3.5
Outputs:
- propagated: float32 [256, 1024, 512], P('gz', 'gx', 'gy')
The draws below stay inside these ranges and needn't reach their ends.
All inputs are finite; a program needn't handle non-finite values.
Results may differ from the reference program's by a relative error of at most 0.00007.
Values sent between devices are 32-bit elements; how exact they have to be, the bound alone decides.
No kernel may reach another device: no remote copies, remote signals or barrier semaphores. Data moves between devices by JAX's collectives and lax.ppermute only.
A program may use at most 64 MiB of HBM per device.

```python
import math
import jax
import jax.numpy as jnp
from jax import lax

N1 = 1024
N2 = 512
N3 = 256


def draw_field(key, part):
    keys = jax.random.split(jax.random.fold_in(key, 10), 4)
    spread = math.log(2.2)
    rising = 0.5 * math.log(3.0)
    scale_three = jnp.exp(jax.random.uniform(keys[0], (N3,), jnp.float32, 0.0, spread) + rising * jnp.arange(N3, dtype=jnp.float32) / N3)
    scale_one = jnp.exp(jax.random.uniform(keys[1], (N1,), jnp.float32, 0.0, spread) + rising * jnp.arange(N1, dtype=jnp.float32) / N1)
    scale_two = jnp.exp(jax.random.uniform(keys[2], (N2,), jnp.float32, 0.0, spread) + rising * jnp.arange(N2, dtype=jnp.float32) / N2)
    noise = jax.random.truncated_normal(keys[3], -6.0, 6.0, (N3, N1, N2), jnp.float32)
    values = 0.25 * noise * scale_three[:, None, None] * scale_one[None, :, None] * scale_two[None, None, :]
    return jnp.clip(values, -48.0, 48.0)


def make_factor(key, order):
    keys = jax.random.split(key, 2)
    diagonal = jnp.exp(jax.random.uniform(keys[0], (order,), jnp.float32, 0.0, math.log(3.0)))
    off_part = jax.random.truncated_normal(keys[1], -4.0, 4.0, (order, order), jnp.float32) * 0.6 * order ** (-0.5)
    return off_part + jnp.diag(diagonal)


def draw_factor_a(key, part):
    return make_factor(jax.random.fold_in(key, 11), N1)


def draw_factor_b(key, part):
    return make_factor(jax.random.fold_in(key, 12), N2)


def draw_factor_c(key, part):
    return make_factor(jax.random.fold_in(key, 13), N3)


def setup_inputs(seed: int = 0) -> dict:
    splits = jax.random.split(jax.random.key(seed), 5)
    field = draw_field(jax.random.fold_in(splits[4], 71), 0)
    factor_a = draw_factor_a(jax.random.fold_in(splits[4], 71), 0)
    factor_b = draw_factor_b(jax.random.fold_in(splits[4], 71), 0)
    factor_c = draw_factor_c(jax.random.fold_in(splits[4], 71), 0)
    return {"field": field, "factor_a": factor_a, "factor_b": factor_b, "factor_c": factor_c}


epsilon = 1e-06
target_ratio = 0.5

def apply_operator(tensor, factor_a, factor_b, factor_c):
    highest = lax.Precision.HIGHEST
    along_one = jnp.einsum('ip,kpj->kij', factor_a, tensor, precision=highest)
    along_two = jnp.einsum('kip,jp->kij', tensor, factor_b, precision=highest)
    along_three = jnp.einsum('kp,pij->kij', factor_c, tensor, precision=highest)
    return along_one + along_two + along_three

def reference(field, factor_a, factor_b, factor_c):
    first_term = apply_operator(field, factor_a, factor_b, factor_c)
    size_field = jnp.sum(field * field)
    size_first = jnp.sum(first_term * first_term)
    step = target_ratio * jnp.sqrt(size_field / (size_first + epsilon))
    second_term = apply_operator(first_term, factor_a, factor_b, factor_c)
    return field - step * first_term + step * step / 2.0 * second_term
```

```python
import functools

import jax
import jax.numpy as jnp
from jax import lax
from jax.experimental import pallas as pl
from jax.experimental.pallas import tpu as pltpu
from jax.sharding import Mesh
from jax.sharding import PartitionSpec as P


GX, GZ = ("zh", "core"), ("zl", "x")
Z = ("zh", "zl")

epsilon = 1e-06
target_ratio = 0.5
f32, bf16 = jnp.float32, jnp.bfloat16
VMEM, SMEM = (pl.BlockSpec(memory_space=s) for s in (pltpu.VMEM, pltpu.SMEM))


def halves(x):
    hi = x.astype(bf16)
    return hi, (x - hi.astype(f32)).astype(bf16)


def split_kernel(x_ref, o_ref, *, flip):
    x = x_ref[...]
    hi, lo = halves(x.T if flip else x)
    o_ref[0] = hi
    o_ref[1] = lo


def split_factor(x, flip):
    n = x.shape[0]
    step = min(n, 256)
    if flip:
        out = pl.BlockSpec((2, n, step), lambda i: (0, 0, i))
    else:
        out = pl.BlockSpec((2, step, n), lambda i: (0, i, 0))
    return pl.pallas_call(
        functools.partial(split_kernel, flip=flip),
        grid=(n // step,),
        in_specs=[pl.BlockSpec((step, n), lambda i: (i, 0))],
        out_specs=out,
        out_shape=jax.ShapeDtypeStruct((2, n, n), bf16),
    )(x)


def call(kernel, shapes, *args, scratch=()):
    single = not isinstance(shapes, list)
    shapes = [shapes] if single else shapes
    out = pl.pallas_call(
        kernel,
        out_shape=[jax.ShapeDtypeStruct(s, f32) for s in shapes],
        in_specs=[SMEM if a.dtype == jnp.int32 else VMEM for a in args],
        out_specs=[VMEM] * len(shapes),
        scratch_shapes=scratch,
    )(*args)
    return out[0] if single else out


def mm(a, b):
    return jnp.dot(a, b, preferred_element_type=f32)


def left3(a_ref, x):
    hi, lo = halves(x)
    return mm(a_ref[0], hi) + (mm(a_ref[0], lo) + mm(a_ref[1], hi))


def plane_apply(xs, at_ref, c_ref):
    n = xs[0].shape[0]
    x = jnp.concatenate(xs, axis=0)
    hi, lo = halves(x)
    along = mm(hi, at_ref[0]) + (mm(lo, at_ref[0]) + mm(hi, at_ref[1]))
    out = []
    for j in range(len(xs)):
        h, l = hi[j * n : (j + 1) * n], lo[j * n : (j + 1) * n]
        across = mm(c_ref[0], h) + (mm(c_ref[0], l) + mm(c_ref[1], h))
        out.append(along[j * n : (j + 1) * n] + across)
    return out


def first_kernel(v_ref, at_ref, c_ref, g_ref):
    n_gy, n_gx, n_gz, n_j, kk, ii = g_ref.shape
    xs = [
        jnp.concatenate(
            [v_ref[gx, :, j].reshape(n_gz * n_gy * kk, ii) for gx in range(n_gx)], axis=1
        )
        for j in range(n_j)
    ]
    for j, y in enumerate(plane_apply(xs, at_ref, c_ref)):
        for gx in range(n_gx):
            part = y[:, gx * ii : (gx + 1) * ii].reshape(n_gz, n_gy, kk, ii)
            for gy in range(n_gy):
                g_ref[gy, gx, :, j] = part[:, gy]


def second_kernel(g_ref, at_ref, c_ref, h_ref):
    n_gy, n_gx, n_gz, n_j, kk, ii = g_ref.shape
    xs = [
        jnp.concatenate(
            [
                jnp.stack([g_ref[gy, gx, :, j] for gy in range(n_gy)], axis=1).reshape(
                    n_gz * n_gy * kk, ii
                )
                for gx in range(n_gx)
            ],
            axis=1,
        )
        for j in range(n_j)
    ]
    for j, y in enumerate(plane_apply(xs, at_ref, c_ref)):
        for gx in range(n_gx):
            h_ref[gx, :, j] = y[:, gx * ii : (gx + 1) * ii].reshape(n_gz, n_gy * kk, ii)


def square_sum(x):
    return jnp.sum((x * x).reshape(-1, 8, 128), axis=0)


def row_kernel(me_ref, *refs):
    *v_refs, b_ref, o_ref, sum_ref, rows_ref = refs
    gy = len(v_refs)
    for d, v in enumerate(v_refs):
        rows_ref[lax.rem(me_ref[0] + gy - d, gy)] = v[...]
    rows = rows_ref[...]
    cols = rows.shape[1]
    sum_ref[...] = square_sum(rows)
    o_ref[...] = left3(b_ref, rows.reshape(gy * cols, -1)).reshape(o_ref.shape)


def term_kernel(me_ref, bv_ref, g_ref, *refs):
    *o_refs, sum_ref = refs
    gy = len(o_refs)
    total = jnp.zeros(sum_ref.shape, f32)
    for d, o in enumerate(o_refs):
        to = lax.rem(me_ref[0] + d, gy)
        value = bv_ref[to] + g_ref[to]
        total += square_sum(value)
        o[...] = value
    sum_ref[...] = total


def cross_kernel(me_ref, bv_ref, g_ref, b_ref, *o_refs):
    gy, cols = g_ref.shape[:2]
    hi, lo = halves((bv_ref[...] + 2.0 * g_ref[...]).reshape(gy * cols, -1))
    for d, o in enumerate(o_refs):
        to = pl.multiple_of(lax.rem(me_ref[0] + d, gy) * cols, cols)
        bh, bl = b_ref[0, pl.ds(to, cols)], b_ref[1, pl.ds(to, cols)]
        o[...] = (mm(bh, hi) + (mm(bh, lo) + mm(bl, hi))).reshape(o.shape)


def last_kernel(me_ref, sum_ref, v_ref, h_ref, *refs):
    *pieces, o_ref = refs
    gy = len(pieces) // 2
    sub = v_ref.shape[0]
    size_field, size_first = jnp.sum(sum_ref[0]), jnp.sum(sum_ref[1])
    ratio = size_field / (jnp.full((1, 128), size_first, f32) + epsilon)
    step = (target_ratio * jnp.sqrt(ratio)).reshape(1, 1, 128)
    for d in range(gy):

        @pl.when(pl.program_id(0) == d)
        def _():
            first, cross = pieces[d], pieces[gy + d]
            value = (step * step / 2.0) * (cross[...] + h_ref[...]) - step * first[...]
            for k in range(sub):
                o_ref[k] = v_ref[k] + value[:, k].T


def last_step(me, sums, field, h, firsts, crosses):
    gy = len(firsts)
    depth, rows, cols = field.shape
    sub = depth // gy
    at = lambda d, me: lax.rem(me[0] + gy - d, gy)
    block = pl.BlockSpec((sub, rows, cols), lambda d, me: (at(d, me), 0, 0))
    turned = pl.BlockSpec((cols, sub, rows), lambda d, me: (0, at(d, me), 0))
    whole = pl.BlockSpec((cols, sub, rows), lambda d, me: (0, 0, 0))
    return pl.pallas_call(
        last_kernel,
        grid_spec=pltpu.PrefetchScalarGridSpec(
            num_scalar_prefetch=1,
            grid=(gy,),
            in_specs=[pl.BlockSpec(sums.shape, lambda d, me: (0, 0, 0)), block, turned]
            + [whole] * (2 * gy),
            out_specs=block,
        ),
        out_shape=jax.ShapeDtypeStruct(field.shape, f32),
    )(me, sums, field, h, *firsts, *crosses)


def on_device(field, factor_a, factor_b, factor_c):
    gx, gy, gz = (lax.axis_size(a) for a in (GX, "gy", GZ))
    depth, rows, cols = field.shape
    me = lax.axis_index("gy")
    me_arg = me.reshape(1)
    sub = depth // gy
    planes = cols // (gx * gz)

    def shifted(value, axis, d):
        n = lax.axis_size(axis)
        return lax.ppermute(value, axis, [(i, (i + d) % n) for i in range(n)])

    def shifted_z(value, d):
        zh, zl = (lax.axis_size(a) for a in Z)
        return shifted(value, Z, d)

    def to_neighbours(pieces):
        return [shifted(p, "gy", d) if d else p for d, p in enumerate(pieces)]

    turned = field.transpose(2, 0, 1)

    there = lax.all_to_all(turned, GX + GZ, 0, 0, tiled=True)
    there = there.reshape(gx, gz, planes, depth, rows)

    at = split_factor(factor_a, True)
    c = split_factor(factor_c, False)
    b = split_factor(factor_b, False)

    pieces = [
        lax.dynamic_slice_in_dim(turned, lax.rem(me + d, gy) * sub, sub, 1) for d in range(gy)
    ]
    bv, size_field = call(
        row_kernel,
        [(gy, cols, sub, rows), (8, 128)],
        me_arg,
        *to_neighbours(pieces),
        b,
        scratch=[pltpu.VMEM((gy, cols, sub, rows), f32)],
    )
    there, bv = lax.optimization_barrier((there, bv))

    g = call(first_kernel, (gy, gx, gz, planes, sub, rows), there, at, c)
    g_rows = lax.all_to_all(g.reshape(-1, sub, rows), ("gy",) + GX + GZ, 0, 0, tiled=True)
    g_rows = g_rows.reshape(gy, cols, sub, rows)
    h = call(second_kernel, (gx, gz, planes, depth, rows), g, at, c)
    g_rows, h = lax.optimization_barrier((g_rows, h))
    h = lax.all_to_all(h.reshape(cols, depth, rows), GX + GZ, 0, 0, tiled=True)

    piece = (cols, sub, rows)
    *first, size_first = call(term_kernel, [piece] * gy + [(8, 128)], me_arg, bv, g_rows)
    sums = jnp.stack([size_field, size_first])
    sums = sums + sum(shifted(sums, "gy", d) for d in range(1, gy))
    first = to_neighbours(first)
    cross = to_neighbours(call(cross_kernel, [piece] * gy, me_arg, bv, g_rows, b))
    sums = sums + shifted(sums, "core", 1)
    sums = sums + sum(shifted(sums, "x", d) for d in range(1, lax.axis_size("x")))
    sums = sums + sum(shifted_z(sums, d) for d in range(1, lax.axis_size(Z)))
    return last_step(me_arg, sums, field, h, first, cross)


def solution(mesh):
    finer = Mesh(
        mesh.devices.reshape(4, 2, mesh.shape["gy"], 2, 4), GX + ("gy",) + GZ
    )
    spec = P(GZ, GX, "gy")
    return jax.shard_map(
        on_device, mesh=finer, in_specs=(spec, P(), P(), P()), out_specs=spec, check_vma=False
    )
```

```python
import functools

import jax
import jax.numpy as jnp
from jax import lax
from jax.experimental import pallas as pl
from jax.experimental.pallas import tpu as pltpu
from jax.sharding import Mesh
from jax.sharding import PartitionSpec as P


GX, GZ = ("zh", "core"), ("zl", "x")
Z = ("zh", "zl")
PLANES = ("core", "zh", "zl", "x")

epsilon = 1e-06
target_ratio = 0.5
f32, bf16 = jnp.float32, jnp.bfloat16
LIMIT = pltpu.CompilerParams(vmem_limit_bytes=32 << 20)
HBM = pltpu.HBM
VMEM, SMEM, ANY, IN_HBM = (
    pl.BlockSpec(memory_space=s) for s in (pltpu.VMEM, pltpu.SMEM, pl.ANY, HBM)
)


def halves(x):
    hi = x.astype(bf16)
    return hi, (x - hi.astype(f32)).astype(bf16)


def split_kernel(x_ref, o_ref, *, flip):
    x = x_ref[...]
    hi, lo = halves(x.T if flip else x)
    if flip:
        o_ref[0, 0], o_ref[0, 1] = hi, lo
    else:
        o_ref[0], o_ref[1] = hi, lo


def split_factor(x, flip=0):
    n = x.shape[0]
    step = flip or n
    if flip:
        shape = (n // flip, 2, n, flip)
        out = pl.BlockSpec((1,) + shape[1:], lambda i: (i, 0, 0, 0))
        shape = HBM(shape, bf16)
    else:
        out = pl.BlockSpec((2, n, n), lambda i: (0, 0, 0))
        shape = jax.ShapeDtypeStruct((2, n, n), bf16)
    return pl.pallas_call(
        functools.partial(split_kernel, flip=flip),
        compiler_params=LIMIT,
        grid=(n // step,),
        in_specs=[pl.BlockSpec((step, n), lambda i: (i, 0))],
        out_specs=out,
        out_shape=shape,
    )(x)


def call(kernel, shapes, *args, scratch=(), own=False):
    single = not isinstance(shapes, list)
    shapes = [shapes] if single else shapes
    out = pl.pallas_call(
        kernel,
        compiler_params=LIMIT,
        out_shape=[
            HBM(s, f32) if own and i == 0 else jax.ShapeDtypeStruct(s, f32)
            for i, s in enumerate(shapes)
        ],
        in_specs=[SMEM if a.dtype == jnp.int32 else VMEM for a in args],
        out_specs=[VMEM] * len(shapes),
        scratch_shapes=scratch,
    )(*args)
    return out[0] if single else out


def mm(a, b):
    return jnp.dot(a, b, preferred_element_type=f32)


def left3(a_ref, x):
    hi, lo = halves(x)
    return mm(a_ref[0], hi) + (mm(a_ref[0], lo) + mm(a_ref[1], hi))


def left3_parts(a_ref, hi, lo):
    return mm(a_ref[0], hi) + (mm(a_ref[0], lo) + mm(a_ref[1], hi))


def planes_product(at_ref, c_ref, x_ref, j, along):
    width = at_ref.shape[3]
    m = c_ref.shape[1]
    k = pl.ds(j * m, m)
    lanes = pl.ds(pl.multiple_of(pl.program_id(0) * width, width), width)
    return along[j * m : (j + 1) * m] + left3_parts(c_ref, x_ref[0, k, lanes], x_ref[1, k, lanes])


def along_one(at_ref, x_ref):
    hi, lo = x_ref[0], x_ref[1]
    return mm(hi, at_ref[0, 0]) + (mm(lo, at_ref[0, 0]) + mm(hi, at_ref[0, 1]))


def put(x_ref, j, m, lane, ii, x):
    hi, lo = halves(x.reshape(m, ii))
    x_ref[0, j * m : (j + 1) * m, lane : lane + ii] = hi
    x_ref[1, j * m : (j + 1) * m, lane : lane + ii] = lo


def first_kernel(v_ref, at_ref, c_ref, g_ref, x_ref):
    n_core, n_zh, n_zl, n_x, n_j, kk, ii = v_ref.shape
    n_gy, sub = g_ref.shape[0], g_ref.shape[6]
    m = n_zl * n_x * kk

    @pl.when(pl.program_id(0) == 0)
    def _():
        for j in range(n_j):
            for z in range(n_zh):
                for c in range(n_core):
                    put(x_ref, j, m, (z * n_core + c) * ii, ii, v_ref[c, z, :, :, j])

    along = along_one(at_ref, x_ref)
    for j in range(n_j):
        y = planes_product(at_ref, c_ref, x_ref, j, along)
        for c in range(n_core):
            part = y[:, c * ii : (c + 1) * ii].reshape(n_zl, n_x, n_gy, sub, ii)
            for gy in range(n_gy):
                g_ref[gy, c, 0, :, :, j] = part[:, :, gy]


def second_kernel(g_ref, at_ref, c_ref, h_ref, x_ref):
    n_gy, n_core, n_zh, n_zl, n_x, n_j, sub, ii = g_ref.shape
    m = n_zl * n_x * n_gy * sub

    @pl.when(pl.program_id(0) == 0)
    def _():
        for j in range(n_j):
            for z in range(n_zh):
                for c in range(n_core):
                    x = jnp.stack([g_ref[gy, c, z, :, :, j] for gy in range(n_gy)], axis=2)
                    put(x_ref, j, m, (z * n_core + c) * ii, ii, x)

    along = along_one(at_ref, x_ref)
    for j in range(n_j):
        y = planes_product(at_ref, c_ref, x_ref, j, along)
        for c in range(n_core):
            h_ref[c, 0, :, :, j] = y[:, c * ii : (c + 1) * ii].reshape(n_zl, n_x, n_gy * sub, ii)


def planes_call(kernel, value, at, c, shape):
    zh = len(shape) - 6
    n, m = at.shape[2], c.shape[1]
    n_zh = shape[zh]
    whole = lambda a: pl.BlockSpec(a.shape, lambda i, nd=a.ndim: (0,) * nd)
    index = lambda i: tuple(i if d == zh else 0 for d in range(len(shape)))
    return pl.pallas_call(
        kernel,
        compiler_params=pltpu.CompilerParams(vmem_limit_bytes=61 << 20),
        grid=(n_zh,),
        in_specs=[whole(value), pl.BlockSpec((1,) + at.shape[1:], lambda i: (i, 0, 0, 0)), whole(c)],
        out_specs=pl.BlockSpec(shape[:zh] + (1,) + shape[zh + 1 :], index),
        out_shape=HBM(shape, f32),
        scratch_shapes=[pltpu.VMEM((2, shape[-3] * m, n), bf16)],
    )(value, at, c)


def y_pack_kernel(me_ref, v_ref, *o_refs):
    n_y = len(o_refs)
    sub = v_ref.shape[1] // n_y
    for d, o in enumerate(o_refs):
        to = pl.multiple_of(lax.rem(me_ref[0] + d, n_y) * sub, sub)
        o[...] = v_ref[:, pl.ds(to, sub)]


def square_sum(x):
    return jnp.sum((x * x).reshape(-1, 8, 128), axis=0)


def row_kernel(me_ref, *refs):
    *v_refs, b_ref, o_ref, sum_ref, rows_ref = refs
    gy = len(v_refs)
    for d, v in enumerate(v_refs):
        rows_ref[lax.rem(me_ref[0] + gy - d, gy)] = v[...]
    rows = rows_ref[...]
    sum_ref[...] = square_sum(rows)
    o_ref[...] = left3(b_ref, rows.reshape(gy * rows.shape[1], -1)).reshape(o_ref.shape)


def term_kernel(me_ref, bv_ref, g_ref, *refs):
    *o_refs, sum_ref = refs
    gy = len(o_refs)
    total = jnp.zeros(sum_ref.shape, f32)
    for d, o in enumerate(o_refs):
        to = lax.rem(me_ref[0] + d, gy)
        value = bv_ref[to] + g_ref[to]
        total += square_sum(value)
        o[...] = value
    sum_ref[...] = total


def cross_kernel(me_ref, bv_ref, g_ref, b_ref, *o_refs):
    gy, cols = bv_ref.shape[:2]
    hi, lo = halves((bv_ref[...] + 2.0 * g_ref[...]).reshape(gy * cols, -1))
    for d, o in enumerate(o_refs):
        to = pl.multiple_of(lax.rem(me_ref[0] + d, gy) * cols, cols)
        bh, bl = b_ref[0, pl.ds(to, cols)], b_ref[1, pl.ds(to, cols)]
        o[...] = (mm(bh, hi) + (mm(bh, lo) + mm(bl, hi))).reshape(o.shape)


def last_kernel(me_ref, sum_ref, v_ref, h_ref, *refs):
    n_y = (len(refs) - 7) // 2
    pieces, o_ref = refs[: 2 * n_y], refs[2 * n_y]
    v_buf, h_buf, p_buf, o_buf, in_sem, out_sem = refs[2 * n_y + 1 :]
    sub = v_buf.shape[1]
    loads, stores = [], []
    for d in range(n_y):
        k = pl.ds(pl.multiple_of(lax.rem(me_ref[0] + n_y - d, n_y) * sub, sub), sub)
        parts = (
            (pieces[d], p_buf.at[d, 0]),
            (pieces[n_y + d], p_buf.at[d, 1]),
            (v_ref.at[k], v_buf.at[d]),
            (h_ref.at[:, k], h_buf.at[d]),
        )
        loads.append(
            [pltpu.make_async_copy(a, b, in_sem.at[d, i]) for i, (a, b) in enumerate(parts)]
        )
        stores.append(pltpu.make_async_copy(o_buf.at[d], o_ref.at[k], out_sem.at[d]))
        for load in loads[-1]:
            load.start()
    size_field, size_first = jnp.sum(sum_ref[0]), jnp.sum(sum_ref[1])
    ratio = size_field / (jnp.full((1, 128), size_first, f32) + epsilon)
    step = (target_ratio * jnp.sqrt(ratio)).reshape(1, 1, 128)
    for d in range(n_y):
        for load in loads[d]:
            load.wait()
        value = (step * step / 2.0) * (p_buf[d, 1] + h_buf[d]) - step * p_buf[d, 0]
        for k in range(sub):
            o_buf[d, k] = v_buf[d, k] + value[:, k].T
        stores[d].start()
    for store in stores:
        store.wait()


def last_step(me, sums, field, h, firsts, crosses):
    n_y = len(crosses)
    depth, rows, cols = field.shape
    sub = depth // n_y
    block, turned = (n_y, sub, rows, cols), (n_y, cols, sub, rows)
    return pl.pallas_call(
        last_kernel,
        compiler_params=pltpu.CompilerParams(vmem_limit_bytes=60 << 20),
        in_specs=[SMEM, VMEM, IN_HBM, ANY] + ([IN_HBM] + [ANY] * (n_y - 1)) * 2,
        out_specs=ANY,
        out_shape=jax.ShapeDtypeStruct(field.shape, f32),
        scratch_shapes=[
            pltpu.VMEM(block, f32),
            pltpu.VMEM(turned, f32),
            pltpu.VMEM((n_y, 2) + turned[1:], f32),
            pltpu.VMEM(block, f32),
            pltpu.SemaphoreType.DMA((n_y, 4)),
            pltpu.SemaphoreType.DMA((n_y,)),
        ],
    )(me, sums, field, h, *firsts, *crosses)


def on_device(field, factor_a, factor_b, factor_c):
    n_y, n_x, n_z = (lax.axis_size(a) for a in ("gy", "x", Z))
    depth, rows, cols = field.shape
    sub = depth // n_y
    me_y = lax.axis_index("gy").reshape(1)
    grid = tuple(lax.axis_size(a) for a in PLANES)
    planes = cols // lax.axis_size(PLANES)

    def shifted(value, axis, d):
        n = lax.axis_size(axis)
        return lax.ppermute(value, axis, [(i, (i + d) % n) for i in range(n)])

    def exchanged(pieces, axis):
        return [shifted(p, axis, d) if d else p for d, p in enumerate(pieces)]

    def all_to_all(value, axes):
        value = value.reshape((-1,) + value.shape[-2:])
        return lax.all_to_all(value, axes, 0, 0, tiled=True)

    turned = field.transpose(2, 0, 1)
    v = all_to_all(turned, PLANES).reshape(grid + (planes, depth, rows))

    piece = (cols, sub, rows)
    rows_in = call(y_pack_kernel, [piece] * n_y, me_y, turned)
    rows_in = exchanged(rows_in, "gy")
    c = split_factor(factor_c)
    at = split_factor(factor_a, lax.axis_size("core") * rows)
    b = split_factor(factor_b)
    bv, size_field = call(
        row_kernel,
        [(n_y,) + piece, (8, 128)],
        me_y,
        *rows_in,
        b,
        scratch=[pltpu.VMEM((n_y,) + piece, f32)],
    )

    g = planes_call(first_kernel, v, at, c, (n_y,) + grid + (planes, sub, rows))
    g_rows = all_to_all(g, ("gy",) + PLANES).reshape(n_y, cols, sub, rows)
    h = planes_call(second_kernel, g, at, c, grid + (planes, depth, rows))
    h = all_to_all(h, PLANES)

    *first, size_first = call(term_kernel, [piece] * n_y + [(8, 128)], me_y, bv, g_rows, own=True)
    sums = jnp.stack([size_field, size_first])
    sums = sums + sum(shifted(sums, "gy", d) for d in range(1, n_y))
    first = exchanged(first, "gy")
    cross = call(cross_kernel, [piece] * n_y, me_y, bv, g_rows, b, own=True)
    cross = exchanged(cross, "gy")
    sums = sums + shifted(sums, "core", 1)
    sums = sums + sum(shifted(sums, "x", d) for d in range(1, n_x))
    sums = sums + sum(shifted(sums, Z, d) for d in range(1, n_z))
    return last_step(me_y, sums, field, h, first, cross)


def solution(mesh):
    finer = Mesh(
        mesh.devices.reshape(4, 2, mesh.shape["gy"], 2, 4), GX + ("gy",) + GZ
    )
    spec = P(GZ, GX, "gy")
    return jax.shard_map(
        on_device, mesh=finer, in_specs=(spec, P(), P(), P()), out_specs=spec, check_vma=False
    )
```

```python
import functools

import jax
import jax.numpy as jnp
from jax import lax
from jax.experimental import pallas as pl
from jax.experimental.pallas import tpu as pltpu
from jax.sharding import Mesh
from jax.sharding import PartitionSpec as P


GX, GZ = ("zh", "core"), ("zl", "x")
Z = ("zh", "zl")
PLANES = ("core", "zh", "zl", "x")

epsilon = 1e-06
target_ratio = 0.5
f32, bf16 = jnp.float32, jnp.bfloat16
LIMIT = pltpu.CompilerParams(vmem_limit_bytes=32 << 20)
HBM = pltpu.HBM
VMEM, SMEM, ANY, IN_HBM = (
    pl.BlockSpec(memory_space=s) for s in (pltpu.VMEM, pltpu.SMEM, pl.ANY, HBM)
)


def far(x):
    return pltpu.with_memory_space_constraint(x, HBM)


def halves(x):
    hi = x.astype(bf16)
    return hi, (x - hi.astype(f32)).astype(bf16)


def split_kernel(x_ref, o_ref, *, flip):
    x = x_ref[...]
    hi, lo = halves(x.T if flip else x)
    if flip:
        o_ref[0, 0], o_ref[0, 1] = hi, lo
    else:
        o_ref[0], o_ref[1] = hi, lo


def split_factor(x, flip=0):
    n = x.shape[0]
    step = flip or n
    if flip:
        shape = (n // flip, 2, n, flip)
        out = pl.BlockSpec((1,) + shape[1:], lambda i: (i, 0, 0, 0))
        shape = HBM(shape, bf16)
    else:
        out = pl.BlockSpec((2, n, n), lambda i: (0, 0, 0))
        shape = jax.ShapeDtypeStruct((2, n, n), bf16)
    return pl.pallas_call(
        functools.partial(split_kernel, flip=flip),
        compiler_params=LIMIT,
        grid=(n // step,),
        in_specs=[pl.BlockSpec((step, n), lambda i: (i, 0))],
        out_specs=out,
        out_shape=shape,
    )(x)


def call(kernel, shapes, *args, scratch=(), own=False):
    single = not isinstance(shapes, list)
    shapes = [shapes] if single else shapes
    out = pl.pallas_call(
        kernel,
        compiler_params=LIMIT,
        out_shape=[
            HBM(s, f32) if own and i == 0 else jax.ShapeDtypeStruct(s, f32)
            for i, s in enumerate(shapes)
        ],
        in_specs=[SMEM if a.dtype == jnp.int32 else VMEM for a in args],
        out_specs=[VMEM] * len(shapes),
        scratch_shapes=scratch,
    )(*args)
    return out[0] if single else out


def mm(a, b):
    return jnp.dot(a, b, preferred_element_type=f32)


def left3(a_ref, x):
    hi, lo = halves(x)
    return mm(a_ref[0], hi) + (mm(a_ref[0], lo) + mm(a_ref[1], hi))


def left3_parts(a_ref, hi, lo):
    return mm(a_ref[0], hi) + (mm(a_ref[0], lo) + mm(a_ref[1], hi))


def planes_product(at_ref, c_ref, x_ref, j, along):
    width = at_ref.shape[3]
    m = c_ref.shape[1]
    k = pl.ds(j * m, m)
    lanes = pl.ds(pl.multiple_of(pl.program_id(0) * width, width), width)
    return along[j * m : (j + 1) * m] + left3_parts(c_ref, x_ref[0, k, lanes], x_ref[1, k, lanes])


def along_one(at_ref, x_ref):
    hi, lo = x_ref[0], x_ref[1]
    return mm(hi, at_ref[0, 0]) + (mm(lo, at_ref[0, 0]) + mm(hi, at_ref[0, 1]))


def put(x_ref, j, m, lane, ii, x):
    hi, lo = halves(x.reshape(m, ii))
    x_ref[0, j * m : (j + 1) * m, lane : lane + ii] = hi
    x_ref[1, j * m : (j + 1) * m, lane : lane + ii] = lo


def first_kernel(v_ref, at_ref, c_ref, g_ref, x_ref):
    n_core, n_zh, n_zl, n_x, n_j, kk, ii = v_ref.shape
    n_gy, sub = g_ref.shape[0], g_ref.shape[6]
    m = n_zl * n_x * kk

    @pl.when(pl.program_id(0) == 0)
    def _():
        for j in range(n_j):
            for z in range(n_zh):
                for c in range(n_core):
                    put(x_ref, j, m, (z * n_core + c) * ii, ii, v_ref[c, z, :, :, j])

    along = along_one(at_ref, x_ref)
    for j in range(n_j):
        y = planes_product(at_ref, c_ref, x_ref, j, along)
        for c in range(n_core):
            part = y[:, c * ii : (c + 1) * ii].reshape(n_zl, n_x, n_gy, sub, ii)
            for gy in range(n_gy):
                g_ref[gy, c, 0, :, :, j] = part[:, :, gy]


def second_kernel(g_ref, at_ref, c_ref, h_ref, x_ref):
    n_gy, n_core, n_zh, n_zl, n_x, n_j, sub, ii = g_ref.shape
    m = n_zl * n_x * n_gy * sub

    @pl.when(pl.program_id(0) == 0)
    def _():
        for j in range(n_j):
            for z in range(n_zh):
                for c in range(n_core):
                    x = jnp.stack([g_ref[gy, c, z, :, :, j] for gy in range(n_gy)], axis=2)
                    put(x_ref, j, m, (z * n_core + c) * ii, ii, x)

    along = along_one(at_ref, x_ref)
    for j in range(n_j):
        y = planes_product(at_ref, c_ref, x_ref, j, along)
        for c in range(n_core):
            h_ref[c, 0, :, :, j] = y[:, c * ii : (c + 1) * ii].reshape(n_zl, n_x, n_gy * sub, ii)


def planes_call(kernel, value, at, c, shape):
    zh = len(shape) - 6
    n, m = at.shape[2], c.shape[1]
    n_zh = shape[zh]
    whole = lambda a: pl.BlockSpec(a.shape, lambda i, nd=a.ndim: (0,) * nd)
    index = lambda i: tuple(i if d == zh else 0 for d in range(len(shape)))
    return pl.pallas_call(
        kernel,
        compiler_params=LIMIT,
        grid=(n_zh,),
        in_specs=[whole(value), pl.BlockSpec((1,) + at.shape[1:], lambda i: (i, 0, 0, 0)), whole(c)],
        out_specs=pl.BlockSpec(shape[:zh] + (1,) + shape[zh + 1 :], index),
        out_shape=HBM(shape, f32),
        scratch_shapes=[pltpu.VMEM((2, shape[-3] * m, n), bf16)],
    )(value, far(at), c)


def y_pack_kernel(me_ref, v_ref, *o_refs):
    n_y = len(o_refs)
    sub = v_ref.shape[1] // n_y
    for d, o in enumerate(o_refs):
        to = pl.multiple_of(lax.rem(me_ref[0] + d, n_y) * sub, sub)
        o[...] = v_ref[:, pl.ds(to, sub)]


def square_sum(x):
    return jnp.sum((x * x).reshape(-1, 8, 128), axis=0)


def row_kernel(me_ref, *refs):
    *v_refs, b_ref, o_ref, sum_ref, rows_ref = refs
    gy = len(v_refs)
    for d, v in enumerate(v_refs):
        rows_ref[lax.rem(me_ref[0] + gy - d, gy)] = v[...]
    rows = rows_ref[...]
    sum_ref[...] = square_sum(rows)
    o_ref[...] = left3(b_ref, rows.reshape(gy * rows.shape[1], -1)).reshape(o_ref.shape)


def term_kernel(me_ref, bv_ref, g_ref, *refs):
    *o_refs, sum_ref = refs
    gy = len(o_refs)
    total = jnp.zeros(sum_ref.shape, f32)
    for d, o in enumerate(o_refs):
        to = lax.rem(me_ref[0] + d, gy)
        value = bv_ref[to] + g_ref[to]
        total += square_sum(value)
        o[...] = value
    sum_ref[...] = total


def cross_kernel(me_ref, bv_ref, g_ref, b_ref, *o_refs):
    gy, cols = bv_ref.shape[:2]
    hi, lo = halves((bv_ref[...] + 2.0 * g_ref[...]).reshape(gy * cols, -1))
    for d, o in enumerate(o_refs):
        to = pl.multiple_of(lax.rem(me_ref[0] + d, gy) * cols, cols)
        bh, bl = b_ref[0, pl.ds(to, cols)], b_ref[1, pl.ds(to, cols)]
        o[...] = (mm(bh, hi) + (mm(bh, lo) + mm(bl, hi))).reshape(o.shape)


def last_kernel(me_ref, sum_ref, v_ref, h_ref, *refs):
    n_y = (len(refs) - 7) // 2
    pieces, o_ref = refs[: 2 * n_y], refs[2 * n_y]
    v_buf, h_buf, p_buf, o_buf, in_sem, out_sem = refs[2 * n_y + 1 :]
    sub = v_buf.shape[1]
    loads, stores = [], []
    for d in range(n_y):
        k = pl.ds(pl.multiple_of(lax.rem(me_ref[0] + n_y - d, n_y) * sub, sub), sub)
        parts = (
            (pieces[d], p_buf.at[d, 0]),
            (pieces[n_y + d], p_buf.at[d, 1]),
            (v_ref.at[k], v_buf.at[d]),
            (h_ref.at[:, k], h_buf.at[d]),
        )
        loads.append(
            [pltpu.make_async_copy(a, b, in_sem.at[d, i]) for i, (a, b) in enumerate(parts)]
        )
        stores.append(pltpu.make_async_copy(o_buf.at[d], o_ref.at[k], out_sem.at[d]))
        for load in loads[-1]:
            load.start()
    size_field, size_first = jnp.sum(sum_ref[0]), jnp.sum(sum_ref[1])
    ratio = size_field / (jnp.full((1, 128), size_first, f32) + epsilon)
    step = (target_ratio * jnp.sqrt(ratio)).reshape(1, 1, 128)
    for d in range(n_y):
        for load in loads[d]:
            load.wait()
        value = (step * step / 2.0) * (p_buf[d, 1] + h_buf[d]) - step * p_buf[d, 0]
        for k in range(sub):
            o_buf[d, k] = v_buf[d, k] + value[:, k].T
        stores[d].start()
    for store in stores:
        store.wait()


def last_step(me, sums, field, h, firsts, crosses):
    n_y = len(crosses)
    depth, rows, cols = field.shape
    sub = depth // n_y
    block, turned = (n_y, sub, rows, cols), (n_y, cols, sub, rows)
    return pl.pallas_call(
        last_kernel,
        compiler_params=LIMIT,
        in_specs=[SMEM, VMEM, IN_HBM, ANY] + ([IN_HBM] + [ANY] * (n_y - 1)) * 2,
        out_specs=ANY,
        out_shape=jax.ShapeDtypeStruct(field.shape, f32),
        scratch_shapes=[
            pltpu.VMEM(block, f32),
            pltpu.VMEM(turned, f32),
            pltpu.VMEM((n_y, 2) + turned[1:], f32),
            pltpu.VMEM(block, f32),
            pltpu.SemaphoreType.DMA((n_y, 4)),
            pltpu.SemaphoreType.DMA((n_y,)),
        ],
    )(me, sums, far(field), far(h), far(firsts[0]), *firsts[1:], far(crosses[0]), *crosses[1:])


def on_device(field, factor_a, factor_b, factor_c):
    n_y, n_x, n_z = (lax.axis_size(a) for a in ("gy", "x", Z))
    depth, rows, cols = field.shape
    sub = depth // n_y
    me_y = lax.axis_index("gy").reshape(1)
    grid = tuple(lax.axis_size(a) for a in PLANES)
    planes = cols // lax.axis_size(PLANES)

    def shifted(value, axis, d):
        n = lax.axis_size(axis)
        return lax.ppermute(value, axis, [(i, (i + d) % n) for i in range(n)])

    def exchanged(pieces, axis):
        return [shifted(p, axis, d) if d else p for d, p in enumerate(pieces)]

    def all_to_all(value, axes):
        value = value.reshape((-1,) + value.shape[-2:])
        return lax.all_to_all(value, axes, 0, 0, tiled=True)

    turned = field.transpose(2, 0, 1)
    v = all_to_all(turned, PLANES).reshape(grid + (planes, depth, rows))

    piece = (cols, sub, rows)
    rows_in = call(y_pack_kernel, [piece] * n_y, me_y, turned)
    rows_in = exchanged(rows_in, "gy")
    c = split_factor(factor_c)
    at = split_factor(factor_a, lax.axis_size("core") * rows)
    b = split_factor(factor_b)
    bv, size_field = call(
        row_kernel,
        [(n_y,) + piece, (8, 128)],
        me_y,
        *rows_in,
        b,
        scratch=[pltpu.VMEM((n_y,) + piece, f32)],
    )

    g = planes_call(first_kernel, v, at, c, (n_y,) + grid + (planes, sub, rows))
    g_rows = all_to_all(g, ("gy",) + PLANES).reshape(n_y, cols, sub, rows)
    h = planes_call(second_kernel, g, at, c, grid + (planes, depth, rows))
    h = all_to_all(h, PLANES)

    *first, size_first = call(term_kernel, [piece] * n_y + [(8, 128)], me_y, bv, g_rows, own=True)
    sums = jnp.stack([size_field, size_first])
    sums = sums + sum(shifted(sums, "gy", d) for d in range(1, n_y))
    first = exchanged(first, "gy")
    cross = call(cross_kernel, [piece] * n_y, me_y, bv, g_rows, b, own=True)
    cross = exchanged(cross, "gy")
    sums = sums + shifted(sums, "core", 1)
    sums = sums + sum(shifted(sums, "x", d) for d in range(1, n_x))
    sums = sums + sum(shifted(sums, Z, d) for d in range(1, n_z))
    return last_step(me_y, sums, field, h, first, cross)


def solution(mesh):
    finer = Mesh(
        mesh.devices.reshape(4, 2, mesh.shape["gy"], 2, 4), GX + ("gy",) + GZ
    )
    spec = P(GZ, GX, "gy")
    return jax.shard_map(
        on_device, mesh=finer, in_specs=(spec, P(), P(), P()), out_specs=spec, check_vma=False
    )
```

```python
import functools

import jax
import jax.numpy as jnp
from jax import lax
from jax.experimental import pallas as pl
from jax.experimental.pallas import tpu as pltpu
from jax.sharding import Mesh
from jax.sharding import PartitionSpec as P


GX, GZ = ("zh", "core"), ("zl", "x")
Z = ("zh", "zl")
PLANES = ("core", "zh", "zl", "x")

epsilon = 1e-06
target_ratio = 0.5
f32, bf16 = jnp.float32, jnp.bfloat16
LIMIT = pltpu.CompilerParams(vmem_limit_bytes=32 << 20)
HBM = pltpu.HBM
VMEM, SMEM, ANY, IN_HBM = (
    pl.BlockSpec(memory_space=s) for s in (pltpu.VMEM, pltpu.SMEM, pl.ANY, HBM)
)


def far(x):
    return pltpu.with_memory_space_constraint(x, HBM)


def halves(x):
    hi = x.astype(bf16)
    return hi, (x - hi.astype(f32)).astype(bf16)


def split_kernel(x_ref, o_ref, *, flip):
    x = x_ref[...]
    hi, lo = halves(x.T if flip else x)
    if flip:
        o_ref[0, 0], o_ref[0, 1] = hi, lo
    else:
        o_ref[0], o_ref[1] = hi, lo


def split_factor(x, flip=0):
    n = x.shape[0]
    step = flip or n
    if flip:
        shape = (n // flip, 2, n, flip)
        out = pl.BlockSpec((1,) + shape[1:], lambda i: (i, 0, 0, 0))
        shape = HBM(shape, bf16)
    else:
        out = pl.BlockSpec((2, n, n), lambda i: (0, 0, 0))
        shape = jax.ShapeDtypeStruct((2, n, n), bf16)
    return pl.pallas_call(
        functools.partial(split_kernel, flip=flip),
        compiler_params=LIMIT,
        grid=(n // step,),
        in_specs=[pl.BlockSpec((step, n), lambda i: (i, 0))],
        out_specs=out,
        out_shape=shape,
    )(x)


def call(kernel, shapes, *args, scratch=(), own=False):
    single = not isinstance(shapes, list)
    shapes = [shapes] if single else shapes
    out = pl.pallas_call(
        kernel,
        compiler_params=LIMIT,
        out_shape=[
            HBM(s, f32) if own and i == 0 else jax.ShapeDtypeStruct(s, f32)
            for i, s in enumerate(shapes)
        ],
        in_specs=[SMEM if a.dtype == jnp.int32 else VMEM for a in args],
        out_specs=[VMEM] * len(shapes),
        scratch_shapes=scratch,
    )(*args)
    return out[0] if single else out


def mm(a, b):
    return jnp.dot(a, b, preferred_element_type=f32)


def left3(a_ref, x):
    hi, lo = halves(x)
    return mm(a_ref[0], hi) + (mm(a_ref[0], lo) + mm(a_ref[1], hi))


def left3_parts(a_ref, hi, lo):
    return mm(a_ref[0], hi) + (mm(a_ref[0], lo) + mm(a_ref[1], hi))


def planes_product(at_ref, c_ref, x_ref, j, along):
    width = at_ref.shape[3]
    m = c_ref.shape[1]
    k = pl.ds(j * m, m)
    lanes = pl.ds(pl.multiple_of(pl.program_id(0) * width, width), width)
    return along[j * m : (j + 1) * m] + left3_parts(c_ref, x_ref[0, k, lanes], x_ref[1, k, lanes])


def along_one(at_ref, x_ref):
    hi, lo = x_ref[0], x_ref[1]
    return mm(hi, at_ref[0, 0]) + (mm(lo, at_ref[0, 0]) + mm(hi, at_ref[0, 1]))


def put(x_ref, j, m, lane, ii, x):
    hi, lo = halves(x.reshape(m, ii))
    x_ref[0, j * m : (j + 1) * m, lane : lane + ii] = hi
    x_ref[1, j * m : (j + 1) * m, lane : lane + ii] = lo


def first_kernel(v_ref, at_ref, c_ref, g_ref, x_ref):
    n_core, n_zh, n_zl, n_x, n_j, kk, ii = v_ref.shape
    n_gy, sub = g_ref.shape[0], g_ref.shape[6]
    m = n_zl * n_x * kk

    @pl.when(pl.program_id(0) == 0)
    def _():
        for j in range(n_j):
            for z in range(n_zh):
                for c in range(n_core):
                    put(x_ref, j, m, (z * n_core + c) * ii, ii, v_ref[c, z, :, :, j])

    along = along_one(at_ref, x_ref)
    for j in range(n_j):
        y = planes_product(at_ref, c_ref, x_ref, j, along)
        for c in range(n_core):
            part = y[:, c * ii : (c + 1) * ii].reshape(n_zl, n_x, n_gy, sub, ii)
            for gy in range(n_gy):
                g_ref[gy, c, 0, :, :, j] = part[:, :, gy]


def second_kernel(g_ref, at_ref, c_ref, h_ref, x_ref):
    n_gy, n_core, n_zh, n_zl, n_x, n_j, sub, ii = g_ref.shape
    m = n_zl * n_x * n_gy * sub

    @pl.when(pl.program_id(0) == 0)
    def _():
        for j in range(n_j):
            for z in range(n_zh):
                for c in range(n_core):
                    x = jnp.stack([g_ref[gy, c, z, :, :, j] for gy in range(n_gy)], axis=2)
                    put(x_ref, j, m, (z * n_core + c) * ii, ii, x)

    along = along_one(at_ref, x_ref)
    for j in range(n_j):
        y = planes_product(at_ref, c_ref, x_ref, j, along)
        for c in range(n_core):
            h_ref[c, 0, :, :, j] = y[:, c * ii : (c + 1) * ii].reshape(n_zl, n_x, n_gy * sub, ii)


def planes_call(kernel, value, at, c, shape):
    zh = len(shape) - 6
    n, m = at.shape[2], c.shape[1]
    n_zh = shape[zh]
    whole = lambda a: pl.BlockSpec(a.shape, lambda i, nd=a.ndim: (0,) * nd)
    index = lambda i: tuple(i if d == zh else 0 for d in range(len(shape)))
    return pl.pallas_call(
        kernel,
        compiler_params=LIMIT,
        grid=(n_zh,),
        in_specs=[whole(value), pl.BlockSpec((1,) + at.shape[1:], lambda i: (i, 0, 0, 0)), whole(c)],
        out_specs=pl.BlockSpec(shape[:zh] + (1,) + shape[zh + 1 :], index),
        out_shape=HBM(shape, f32),
        scratch_shapes=[pltpu.VMEM((2, shape[-3] * m, n), bf16)],
    )(value, far(at), c)


def y_pack_kernel(me_ref, v_ref, *o_refs):
    n_y = len(o_refs)
    sub = v_ref.shape[1] // n_y
    for d, o in enumerate(o_refs):
        to = pl.multiple_of(lax.rem(me_ref[0] + d, n_y) * sub, sub)
        o[...] = v_ref[:, pl.ds(to, sub)]


def square_sum(x):
    return jnp.sum((x * x).reshape(-1, 8, 128), axis=0)


def row_kernel(me_ref, *refs):
    *v_refs, b_ref, o_ref, sum_ref, rows_ref = refs
    gy = len(v_refs)
    for d, v in enumerate(v_refs):
        rows_ref[lax.rem(me_ref[0] + gy - d, gy)] = v[...]
    rows = rows_ref[...]
    sum_ref[...] = square_sum(rows)
    o_ref[...] = left3(b_ref, rows.reshape(gy * rows.shape[1], -1)).reshape(o_ref.shape)


def term_kernel(me_ref, bv_ref, g_ref, *refs):
    *o_refs, sum_ref = refs
    gy = len(o_refs)
    total = jnp.zeros(sum_ref.shape, f32)
    for d, o in enumerate(o_refs):
        to = lax.rem(me_ref[0] + d, gy)
        value = bv_ref[to] + g_ref[to]
        total += square_sum(value)
        o[...] = value
    sum_ref[...] = total


def cross_kernel(me_ref, bv_ref, g_ref, b_ref, *o_refs):
    gy, cols = bv_ref.shape[:2]
    hi, lo = halves((bv_ref[...] + 2.0 * g_ref[...]).reshape(gy * cols, -1))
    for d, o in enumerate(o_refs):
        to = pl.multiple_of(lax.rem(me_ref[0] + d, gy) * cols, cols)
        bh, bl = b_ref[0, pl.ds(to, cols)], b_ref[1, pl.ds(to, cols)]
        o[...] = (mm(bh, hi) + (mm(bh, lo) + mm(bl, hi))).reshape(o.shape)


def step_length(sum_ref):
    size_field, size_first = jnp.sum(sum_ref[0]), jnp.sum(sum_ref[1])
    ratio = size_field / (jnp.full((1, 128), size_first, f32) + epsilon)
    return (target_ratio * jnp.sqrt(ratio)).reshape(1, 1, 128)


def home_rows(me_ref, d, n_y, sub):
    return pl.ds(pl.multiple_of(lax.rem(me_ref[0] + n_y - d, n_y) * sub, sub), sub)


def most_kernel(me_ref, sum_ref, v_ref, h_ref, cross_ref, *refs):
    *pieces, o_ref, most_ref, v_buf, h_buf, p_buf, c_buf, o_buf, in_sem, out_sem = refs
    n_y = len(pieces)
    sub = v_buf.shape[1]
    loads = []
    for d in range(n_y):
        k = home_rows(me_ref, d, n_y, sub)
        parts = [
            (pieces[d], p_buf.at[d]),
            (v_ref.at[k], v_buf.at[d]),
            (h_ref.at[:, k], h_buf.at[d]),
        ]
        if d == 0:
            parts.append((cross_ref, c_buf))
        loads.append(
            [pltpu.make_async_copy(a, b, in_sem.at[d, i]) for i, (a, b) in enumerate(parts)]
        )
        for load in loads[-1]:
            load.start()
    step = step_length(sum_ref)
    store = pltpu.make_async_copy(o_buf, o_ref.at[home_rows(me_ref, 0, n_y, sub)], out_sem.at[0])
    for d in range(n_y):
        for load in loads[d]:
            load.wait()
        second = h_buf[d] + c_buf[...] if d == 0 else h_buf[d]
        value = (step * step / 2.0) * second - step * p_buf[d]
        for k in range(sub):
            row = v_buf[d, k] + value[:, k].T
            if d == 0:
                o_buf[k] = row
            else:
                most_ref[d - 1, k] = row
        if d == 0:
            store.start()
    store.wait()


def last_kernel(me_ref, sum_ref, most_ref, part_ref, *refs):
    n_y, sub = most_ref.shape[0] + 1, most_ref.shape[1]
    pieces, (o_ref, p_buf, o_buf, in_sem, out_sem) = refs[: n_y - 1], refs[n_y - 1 :]
    loads = [
        pltpu.make_async_copy(p, p_buf.at[d], in_sem.at[d]) for d, p in enumerate(pieces)
    ]
    for load in loads:
        load.start()
    step = step_length(sum_ref)
    stores = []
    for d in range(n_y - 1):
        loads[d].wait()
        value = (step * step / 2.0) * p_buf[d]
        for k in range(sub):
            o_buf[d, k] = most_ref[d, k] + value[:, k].T
        k = home_rows(me_ref, d + 1, n_y, sub)
        stores.append(pltpu.make_async_copy(o_buf.at[d], o_ref.at[k], out_sem.at[d]))
        stores[-1].start()
    for store in stores:
        store.wait()


def last_step(me, sums, field, h, firsts, crosses):
    n_y = len(crosses)
    depth, rows, cols = field.shape
    sub = depth // n_y
    block, turned = (sub, rows, cols), (cols, sub, rows)
    part, most = pl.pallas_call(
        most_kernel,
        compiler_params=LIMIT,
        in_specs=[SMEM, VMEM, IN_HBM, ANY, IN_HBM, IN_HBM] + [ANY] * (n_y - 1),
        out_specs=[IN_HBM, VMEM],
        out_shape=[
            HBM(field.shape, f32),
            jax.ShapeDtypeStruct((n_y - 1,) + block, f32),
        ],
        scratch_shapes=[
            pltpu.VMEM((n_y,) + block, f32),
            pltpu.VMEM((n_y,) + turned, f32),
            pltpu.VMEM((n_y,) + turned, f32),
            pltpu.VMEM(turned, f32),
            pltpu.VMEM(block, f32),
            pltpu.SemaphoreType.DMA((n_y, 4)),
            pltpu.SemaphoreType.DMA((1,)),
        ],
    )(me, sums, far(field), far(h), far(crosses[0]), far(firsts[0]), *firsts[1:])
    return pl.pallas_call(
        last_kernel,
        compiler_params=LIMIT,
        in_specs=[SMEM, VMEM, VMEM, IN_HBM] + [ANY] * (n_y - 1),
        out_specs=IN_HBM,
        out_shape=HBM(field.shape, f32),
        input_output_aliases={3: 0},
        scratch_shapes=[
            pltpu.VMEM((n_y - 1,) + turned, f32),
            pltpu.VMEM((n_y - 1,) + block, f32),
            pltpu.SemaphoreType.DMA((n_y - 1,)),
            pltpu.SemaphoreType.DMA((n_y - 1,)),
        ],
    )(me, sums, most, part, *crosses[1:])


def on_device(field, factor_a, factor_b, factor_c):
    n_y, n_x, n_z = (lax.axis_size(a) for a in ("gy", "x", Z))
    depth, rows, cols = field.shape
    sub = depth // n_y
    me_y = lax.axis_index("gy").reshape(1)
    grid = tuple(lax.axis_size(a) for a in PLANES)
    planes = cols // lax.axis_size(PLANES)

    def shifted(value, axis, d):
        n = lax.axis_size(axis)
        return lax.ppermute(value, axis, [(i, (i + d) % n) for i in range(n)])

    def exchanged(pieces, axis):
        out = list(pieces)
        for d in sorted(range(1, len(pieces)), key=lambda d: min(d, len(pieces) - d)):
            out[d] = shifted(pieces[d], axis, d)
        return out

    def all_to_all(value, axes):
        value = value.reshape((-1,) + value.shape[-2:])
        return lax.all_to_all(value, axes, 0, 0, tiled=True)

    turned = field.transpose(2, 0, 1)
    v = all_to_all(turned, PLANES).reshape(grid + (planes, depth, rows))

    piece = (cols, sub, rows)
    rows_in = call(y_pack_kernel, [piece] * n_y, me_y, turned)
    rows_in = exchanged(rows_in, "gy")
    c = split_factor(factor_c)
    at = split_factor(factor_a, lax.axis_size("core") * rows)
    b = split_factor(factor_b)
    bv, size_field = call(
        row_kernel,
        [(n_y,) + piece, (8, 128)],
        me_y,
        *rows_in,
        b,
        scratch=[pltpu.VMEM((n_y,) + piece, f32)],
    )

    g = planes_call(first_kernel, v, at, c, (n_y,) + grid + (planes, sub, rows))
    g_rows = all_to_all(g, ("gy",) + PLANES).reshape(n_y, cols, sub, rows)
    h = planes_call(second_kernel, g, at, c, grid + (planes, depth, rows))
    h = all_to_all(h, PLANES)

    *first, size_first = call(term_kernel, [piece] * n_y + [(8, 128)], me_y, bv, g_rows, own=True)
    sums = jnp.stack([size_field, size_first])
    sums = sums + sum(shifted(sums, "gy", d) for d in range(1, n_y))
    first = exchanged(first, "gy")
    cross = call(cross_kernel, [piece] * n_y, me_y, bv, g_rows, b, own=True)
    cross = exchanged(cross, "gy")
    sums = sums + shifted(sums, "core", 1)
    sums = sums + sum(shifted(sums, "x", d) for d in range(1, n_x))
    sums = sums + sum(shifted(sums, Z, d) for d in range(1, n_z))
    return last_step(me_y, sums, field, h, first, cross)


def solution(mesh):
    finer = Mesh(
        mesh.devices.reshape(4, 2, mesh.shape["gy"], 2, 4), GX + ("gy",) + GZ
    )
    spec = P(GZ, GX, "gy")
    return jax.shard_map(
        on_device, mesh=finer, in_specs=(spec, P(), P(), P()), out_specs=spec, check_vma=False
    )
```
